32 devices in a mesh: member: 2 (over y), gx: 4 (over z), gy: 4 (over x, core).
Axes of the slice: x: 2, y: 2, z: 4, core: 2. Of those that a mesh axis runs over, the one named last changes fastest.
Arguments:
- populations: float32 [19, 32, 64, 128], P(None, ('member', 'gx'), 'gy'), parts along dimension 1, may hold values from 0 to 1, as said below
- heat_level: int32 [32, 64, 128], P(('member', 'gx'), 'gy'), parts along dimension 0, may hold values from 0 to 7
- obstacle: int32 [32, 64, 128], P(('member', 'gx'), 'gy'), parts along dimension 0, may hold values 0 or 1
- heat_table: float32 [8], replicated, may hold values from 0.02 to 0.5
Outputs:
- final_populations: float32 [19, 32, 64, 128], P(None, ('member', 'gx'), 'gy'), parts along dimension 1
- velocity: float32 [3, 32, 64, 128], P(None, ('member', 'gx'), 'gy'), parts along dimension 1
The draws below stay inside these ranges and needn't reach their ends.
There are 2 independent parts, one for each index of `member`. The reference program is written for one: setup_inputs(seed, part) draws one part's arguments, and reference() takes and returns one part's arrays. A program takes and returns all parts, laid end to end along the dimension named above; an argument that names none is the same for every part. Nothing has to cross between parts.
Inputs may be any that keep to these rules, and one draw needn't show every extreme that they name: Positive populations near a local equilibrium, in the direction order of the steps.
All inputs are finite; a program needn't handle non-finite values. No bound on the sum of `obstacle` on one device may be relied on, other than what follows from the above.
Results may differ from the reference program's by a relative error of at most 0.0001.
Values sent between devices are 32-bit elements; how exact they have to be, the bound alone decides.
A program may use at most 64 MiB of HBM per device.

```python
import math
import jax
import jax.numpy as jnp
import numpy as np
from jax import lax

NZ = 128
STEPS = 2
LEVELS = 8
NX = 16
NY = 64


lattice = np.array([[0, 0, 0], [1, 0, 0], [-1, 0, 0], [0, 1, 0], [0, -1, 0], [0, 0, 1], [0, 0, -1], [1, 1, 0], [-1, -1, 0], [1, -1, 0], [-1, 1, 0], [1, 0, 1], [-1, 0, -1], [1, 0, -1], [-1, 0, 1], [0, 1, 1], [0, -1, -1], [0, 1, -1], [0, -1, 1]])


lattice_weight = [1.0 / 3.0] + [1.0 / 18.0] * 6 + [1.0 / 36.0] * 12


def draw_populations(key, part):
    key_one, key_two, key_three, key_four, key_five, key_six, key_seven = jax.random.split(jax.random.fold_in(key, 11), 7)
    grid_x = lax.broadcasted_iota(jnp.float32, (NX, NY, NZ), 0)
    grid_y = lax.broadcasted_iota(jnp.float32, (NX, NY, NZ), 1)
    amplitude = jnp.exp(jax.random.uniform(key_four, (), jnp.float32, math.log(0.01), math.log(0.03)))
    speed_ramp = amplitude * (1.0 + grid_x / NX + grid_y / NY)
    sample = jnp.clip(jax.random.normal(key_one, (3, NX, NY, NZ), jnp.float32), -2.5, 2.5)
    density = 1.0 + jax.random.uniform(key_two, (NX, NY, NZ), jnp.float32, -0.05, 0.05)
    velocity = sample * speed_ramp[None]
    plant_speed = jax.random.uniform(key_five, (), jnp.float32, 0.15, 0.4)
    plant_angle = jax.random.uniform(key_six, (), jnp.float32, -math.pi, math.pi)
    key_cx, key_cy, key_cz = jax.random.split(key_seven, 3)
    centre_x = jax.random.randint(key_cx, (), 2, NX - 2)
    centre_y = jax.random.randint(key_cy, (), 3, NY - 3)
    centre_z = jax.random.randint(key_cz, (), 3, NZ - 3)
    index_x = lax.broadcasted_iota(jnp.int32, (NX, NY, NZ), 0)
    index_y = lax.broadcasted_iota(jnp.int32, (NX, NY, NZ), 1)
    index_z = lax.broadcasted_iota(jnp.int32, (NX, NY, NZ), 2)
    region = (jnp.abs(index_x - centre_x) <= 2) & (jnp.abs(index_y - centre_y) <= 2) & (jnp.abs(index_z - centre_z) <= 2)
    planted = plant_speed * jnp.stack([0.9 * jnp.cos(plant_angle), 0.9 * jnp.sin(plant_angle), jnp.float32(0.436)])
    velocity = jnp.where(region[None], planted[:, None, None, None], velocity)
    jitter = jnp.clip(jax.random.normal(key_three, (19, NX, NY, NZ), jnp.float32), -3.0, 3.0)
    speed_sq = velocity[0] * velocity[0] + velocity[1] * velocity[1] + velocity[2] * velocity[2]
    pieces = []
    for number in range(19):
        project = float(lattice[number][0]) * velocity[0] + float(lattice[number][1]) * velocity[1] + float(lattice[number][2]) * velocity[2]
        equilibrium = lattice_weight[number] * density * (1.0 + 3.0 * project + 4.5 * project * project - 1.5 * speed_sq)
        pieces.append(equilibrium * (1.0 + 0.05 * jitter[number]))
    return jnp.stack(pieces).astype(jnp.float32)


def with_ends(values, own_key, least, top_value):
    index_at = [jax.random.randint(jax.random.fold_in(own_key, axis), (), 0, length) for axis, length in enumerate(values.shape)]
    main_axis = values.shape.index(max(values.shape))
    next_to = index_at[:main_axis] + [(index_at[main_axis] + 1) % values.shape[main_axis]] + index_at[main_axis + 1:]
    return values.at[tuple(index_at)].set(least).at[tuple(next_to)].set(top_value)


def setup_inputs(seed: int = 0, part: int = 0) -> dict:
    key_of = jax.random.split(jax.random.key(seed), 5)
    own_keys = jax.random.split(jax.random.fold_in(key_of[4], part), 5)
    populations = draw_populations(jax.random.fold_in(jax.random.fold_in(key_of[4], part), 71), part)
    heat_level = with_ends(jax.random.randint(own_keys[1], (NX, NY, NZ), 0, LEVELS), jax.random.fold_in(own_keys[1], 1), 0, LEVELS - 1).astype(jnp.int32)
    obstacle = with_ends((jax.random.randint(own_keys[2], (NX, NY, NZ), 0, 10) < 1).astype(jnp.int32), jax.random.fold_in(own_keys[2], 1), 0, 1)
    heat_table = jnp.clip(jnp.exp(jax.random.uniform(key_of[3], (LEVELS,), jnp.float32, math.log(0.02), math.log(0.5))), 0.02, 0.5)
    return {"populations": populations, "heat_level": heat_level, "obstacle": obstacle, "heat_table": heat_table}


lattice = np.array([[0, 0, 0], [1, 0, 0], [-1, 0, 0], [0, 1, 0], [0, -1, 0], [0, 0, 1], [0, 0, -1], [1, 1, 0], [-1, -1, 0], [1, -1, 0], [-1, 1, 0], [1, 0, 1], [-1, 0, -1], [1, 0, -1], [-1, 0, 1], [0, 1, 1], [0, -1, -1], [0, 1, -1], [0, -1, 1]])
lattice_weight = [1.0 / 3.0] + [1.0 / 18.0] * 6 + [1.0 / 36.0] * 12
opposite = [0, 2, 1, 4, 3, 6, 5, 8, 7, 10, 9, 12, 11, 14, 13, 16, 15, 18, 17]
base_tau = 0.52
smag_coef = 0.04
speed_cap = 0.1
strain_floor = 1e-06

def stream_all(padded, span_x, span_y, depth_z):
    pieces = []
    for number in range(19):
        shift_x = int(lattice[number][0])
        shift_y = int(lattice[number][1])
        shift_z = int(lattice[number][2])
        pieces.append(padded[number, 1 - shift_x:1 - shift_x + span_x, 1 - shift_y:1 - shift_y + span_y, 1 - shift_z:1 - shift_z + depth_z])
    return jnp.stack(pieces)

def moments(read, solid):
    density = lax.optimization_barrier(jnp.sum(read, axis=0))
    components = []
    for component in range(3):
        moment = jnp.zeros(density.shape, jnp.float32)
        for number in range(19):
            factor = int(lattice[number][component])
            if factor != 0:
                moment = moment + float(factor) * read[number]
        components.append(moment)
    momentum = jnp.stack(components)
    safe_density = jnp.where(solid, 1.0, density)
    velocity = jnp.where(solid[None], 0.0, momentum / safe_density[None])
    return (density, velocity)

def strain_size(vel_wide):
    padded = jnp.pad(vel_wide, ((0, 0), (0, 0), (0, 0), (1, 1)))
    gradient = [(padded[:, 2:, 1:-1, 1:-1] - padded[:, :-2, 1:-1, 1:-1]) * 0.5, (padded[:, 1:-1, 2:, 1:-1] - padded[:, 1:-1, :-2, 1:-1]) * 0.5, (padded[:, 1:-1, 1:-1, 2:] - padded[:, 1:-1, 1:-1, :-2]) * 0.5]
    strain_sum = jnp.zeros(gradient[0].shape[1:], jnp.float32)
    for row_axis in range(3):
        for col_axis in range(3):
            strain_ab = 0.5 * (gradient[col_axis][row_axis] + gradient[row_axis][col_axis])
            strain_sum = strain_sum + strain_ab * strain_ab
    return jnp.sqrt(2.0 * strain_sum + strain_floor)

def collide(read, density, velocity, solid, magnitude, lift_force):
    relax_time = base_tau + 3.0 * smag_coef * magnitude
    speed_sq = velocity[0] * velocity[0] + velocity[1] * velocity[1] + velocity[2] * velocity[2]
    collided = []
    for number in range(19):
        project = float(lattice[number][0]) * velocity[0] + float(lattice[number][1]) * velocity[1] + float(lattice[number][2]) * velocity[2]
        equilibrium = lattice_weight[number] * density * (1.0 + 3.0 * project + 4.5 * project * project - 1.5 * speed_sq)
        fluid_post = read[number] - (read[number] - equilibrium) / relax_time + 3.0 * lattice_weight[number] * float(lattice[number][2]) * lift_force
        collided.append(jnp.where(solid, read[opposite[number]], fluid_post))
    return jnp.stack(collided)

def lookup(heat_level, heat_table):
    heat_force = jnp.zeros(heat_level.shape, jnp.float32)
    for level_no in range(heat_table.shape[0]):
        heat_force = heat_force + jnp.where(heat_level == level_no, heat_table[level_no], 0.0)
    return heat_force

def reference(populations, heat_level, obstacle, heat_table):
    grid_y = lax.broadcasted_iota(jnp.int32, (NX, NY, NZ), 1)
    grid_z = lax.broadcasted_iota(jnp.int32, (NX, NY, NZ), 2)
    solid = (obstacle == 1) | (grid_y == 0) | (grid_y == NY - 1) | (grid_z == 0) | (grid_z == NZ - 1)
    heat_force = lookup(heat_level, heat_table)
    current = populations
    velocity = jnp.zeros((3, NX, NY, NZ), jnp.float32)
    for repeat in range(STEPS):
        padded = jnp.pad(current, ((0, 0), (1, 1), (0, 0), (0, 0)), mode='wrap')
        padded = jnp.pad(padded, ((0, 0), (0, 0), (1, 1), (1, 1)))
        read = stream_all(padded, NX, NY, NZ)
        density, velocity = moments(read, solid)
        peak_speed = jnp.max(velocity[0] * velocity[0] + velocity[1] * velocity[1] + velocity[2] * velocity[2])
        force_scale = speed_cap / jnp.sqrt(speed_cap * speed_cap + peak_speed)
        vel_wide = jnp.pad(velocity, ((0, 0), (1, 1), (0, 0), (0, 0)), mode='wrap')
        vel_wide = jnp.pad(vel_wide, ((0, 0), (0, 0), (1, 1), (0, 0)))
        magnitude = strain_size(vel_wide)
        current = collide(read, density, velocity, solid, magnitude, force_scale * heat_force)
    return (current, velocity)
```

```python
import functools

import jax
import jax.numpy as jnp
import numpy as np
from jax import lax
from jax.experimental import pallas as pl
from jax.experimental.pallas import tpu as pltpu
from jax.sharding import PartitionSpec as P

STEPS = 2
ROW = 8

lattice = np.array(
    [
        [0, 0, 0],
        [1, 0, 0],
        [-1, 0, 0],
        [0, 1, 0],
        [0, -1, 0],
        [0, 0, 1],
        [0, 0, -1],
        [1, 1, 0],
        [-1, -1, 0],
        [1, -1, 0],
        [-1, 1, 0],
        [1, 0, 1],
        [-1, 0, -1],
        [1, 0, -1],
        [-1, 0, 1],
        [0, 1, 1],
        [0, -1, -1],
        [0, 1, -1],
        [0, -1, 1],
    ]
)
CS = [tuple(int(c) for c in row) for row in lattice]
WEIGHT = [1.0 / 3.0] + [1.0 / 18.0] * 6 + [1.0 / 36.0] * 12
OPP = [0, 2, 1, 4, 3, 6, 5, 8, 7, 10, 9, 12, 11, 14, 13, 16, 15, 18, 17]
base_tau = 0.52
smag_coef = 0.04
speed_cap = 0.1
strain_floor = 1e-06
LIFTED = [k for k in range(19) if CS[k][2] != 0]
FLAT = [k for k in range(19) if CS[k][2] == 0]


def tree_sum(items):
    items = list(items)
    while len(items) > 1:
        items = [items[i] + items[i + 1] if i + 1 < len(items) else items[i] for i in range(0, len(items), 2)]
    return items[0]


def kernel(
    ngx, ngy,
    pops, heat_level, obstacle, table,
    out_p, out_v,
    st0, st1, rd, rho_s, v0, v1, hl, ob, solid_s, obuf, pm_src, pm_gy, pm_gx,
    load_sem, a_send, a_recv, b_send, b_recv, p_send, p_recv, out_sem,
):
    _, sx, sy, nz = pops.shape
    levels = table.shape[0]
    gx = lax.axis_index("gx")
    gy = lax.axis_index("gy")
    has_up = gy < ngy - 1
    has_down = gy > 0
    right = lax.rem(gx + 1, ngx)
    left = lax.rem(gx + ngx - 1, ngx)
    own_x = pl.ds(1, sx)
    own_y = pl.ds(ROW, sy)
    top = pl.ds(ROW + sy - 1, 1)
    bottom = pl.ds(ROW, 1)
    rim_low = pl.ds(ROW - 1, 1)
    rim_high = pl.ds(ROW + sy, 1)

    load_p = pltpu.make_async_copy(pops, st0.at[:, own_x, own_y, :], load_sem.at[0])
    load_h = pltpu.make_async_copy(heat_level, hl, load_sem.at[1])
    load_o = pltpu.make_async_copy(obstacle, ob, load_sem.at[2])
    load_p.start()
    load_h.start()
    load_o.start()

    barrier = pltpu.get_barrier_semaphore()

    def greet(x, y):
        pl.semaphore_signal(barrier, inc=1, device_id={"gx": x, "gy": y}, device_id_type=pl.DeviceIdType.MESH)

    for d in range(1, ngx):
        greet(lax.rem(gx + d, ngx), gy)
    for d in range(1, ngy):
        greet(gx, lax.rem(gy + d, ngy))

    @pl.when(has_up)
    def _():
        greet(right, gy + 1)
        greet(left, gy + 1)

    @pl.when(has_down)
    def _():
        greet(right, gy - 1)
        greet(left, gy - 1)

    def zero_rim(rows):
        for ref in (st0, st1, v0, v1):
            ref[:, :, rows, :] = jnp.zeros((ref.shape[0], sx + 2, 1, nz), jnp.float32)

    @pl.when(jnp.logical_not(has_down))
    def _():
        zero_rim(rim_low)

    @pl.when(jnp.logical_not(has_up))
    def _():
        zero_rim(rim_high)

    sides = (
        (None, right, gy, (1, 0)),
        (None, left, gy, (-1, 0)),
        (has_up, gx, gy + 1, (0, 1)),
        (has_down, gx, gy - 1, (0, -1)),
        (has_up, right, gy + 1, (1, 1)),
        (has_down, left, gy - 1, (-1, -1)),
        (has_down, right, gy - 1, (1, -1)),
        (has_up, left, gy + 1, (-1, 1)),
    )
    arrives = (None, None, has_down, has_up, has_down, has_up, has_up, has_down)

    def src_dst(direction):
        dx, dy = direction
        xs = {1: (sx, 0), -1: (1, sx + 1), 0: (own_x, own_x)}[dx]
        ys = {1: (top, rim_low), -1: (bottom, rim_high), 0: (own_y, own_y)}[dy]
        return (xs[0], ys[0]), (xs[1], ys[1])

    def guarded(cond, fn):
        if cond is None:
            fn()
        else:
            pl.when(cond)(fn)

    def moving(direction):
        dx, dy = direction
        if dx and dy:
            return [k for k in range(19) if CS[k][:2] == direction]
        return [k for k in range(19) if (CS[k][0] == dx if dx else CS[k][1] == dy)]

    def exchange(ref, send, recv, many, groups):
        def start(number, x, y, direction):
            def go():
                s, d = src_dst(direction)
                for g in groups(direction):
                    pltpu.make_async_remote_copy(
                        src_ref=ref.at[g, s[0], s[1], :],
                        dst_ref=ref.at[g, d[0], d[1], :],
                        send_sem=send.at[number],
                        recv_sem=recv.at[number],
                        device_id={"gx": x, "gy": y},
                        device_id_type=pl.DeviceIdType.MESH,
                    ).start()
            return go

        for number, (cond, x, y, direction) in enumerate(sides[:many]):
            guarded(cond, start(number, x, y, direction))

        def total(number, direction, sem):
            def go():
                s, _ = src_dst(direction)
                gs = groups(direction)
                view = ref.at[pl.ds(0, len(gs)) if isinstance(gs[0], int) else gs[0], s[0], s[1], :]
                pltpu.make_async_copy(view, view, sem.at[number]).wait()
            return go

        def wait_recv():
            for number in range(many):
                guarded(arrives[number], total(number, sides[number][3], recv))

        def wait_send():
            for number in range(many):
                guarded(sides[number][0], total(number, sides[number][3], send))

        return wait_recv, wait_send

    def spread(step, phase, value, buf):
        count = buf.shape[1]
        pm_src[step, phase] = value
        for d in range(1, count + 1):
            place = {"gy": lax.rem(gy + d, ngy)} if phase == 0 else {"gx": lax.rem(gx + d, ngx)}
            pltpu.make_async_remote_copy(
                src_ref=pm_src.at[step, phase],
                dst_ref=buf.at[step, d - 1],
                send_sem=p_send.at[step, phase],
                recv_sem=p_recv.at[step, phase],
                device_id=place,
                device_id_type=pl.DeviceIdType.MESH,
            ).start()

        def wait():
            pltpu.make_async_copy(buf.at[step], buf.at[step], p_recv.at[step, phase]).wait()
            best = value
            for d in range(count):
                best = jnp.maximum(best, buf[step, d])
            return best

        def wait_send():
            pltpu.make_async_copy(buf.at[step], buf.at[step], p_send.at[step, phase]).wait()

        return wait, wait_send

    blocks = [(x, r) for x in range(sx) for r in range(0, sy, ROW)]
    lane = lax.broadcasted_iota(jnp.int32, (ROW, nz), 1)
    first_lane = lane == 0
    last_lane = lane == nz - 1

    def streamed(st, fs):
        peak = jnp.zeros((ROW, nz), jnp.float32)
        vel = v0 if st is st0 else v1
        for x, r in blocks:
            reads = []
            for k, (cx, cy, cz) in enumerate(CS):
                rows = pl.ds(ROW + r - cy, ROW)
                cells = st[k, x + 1 - cx, rows, :]
                if cz:
                    if fs is not None:
                        cells = cells + (3.0 * WEIGHT[k] * cz) * (fs * v0[3, x + 1 - cx, rows, :])
                    cells = pltpu.roll(cells, cz % nz, 1)
                    cells = jnp.where(first_lane if cz > 0 else last_lane, 0.0, cells)
                rd[k, x, pl.ds(r, ROW), :] = cells
                reads.append(cells)
            density = tree_sum(reads)
            solid = solid_s[x, pl.ds(r, ROW), :] != 0
            inv = jnp.where(solid, 0.0, 1.0 / jnp.where(solid, 1.0, density))
            rho_s[x, pl.ds(r, ROW), :] = density
            speed = []
            for c in range(3):
                plus = tree_sum([reads[k] for k in range(19) if CS[k][c] > 0])
                minus = tree_sum([reads[k] for k in range(19) if CS[k][c] < 0])
                u = (plus - minus) * inv
                vel[c, x + 1, pl.ds(ROW + r, ROW), :] = u
                speed.append(u * u)
            peak = jnp.maximum(peak, speed[0] + speed[1] + speed[2])
        return peak

    def collided(vel, store):
        for x, r in blocks:
            mid = pl.ds(ROW + r, ROW)
            u = [vel[c, x + 1, mid, :] for c in range(3)]
            diff = []
            for a in range(3):
                diff.append(
                    (
                        vel[a, x + 2, mid, :] - vel[a, x, mid, :],
                        vel[a, x + 1, pl.ds(ROW + r + 1, ROW), :] - vel[a, x + 1, pl.ds(ROW + r - 1, ROW), :],
                        pltpu.roll(u[a], nz - 1, 1) - pltpu.roll(u[a], 1, 1),
                    )
                )
            own = diff[0][0] * diff[0][0] + diff[1][1] * diff[1][1] + diff[2][2] * diff[2][2]
            xy = diff[0][1] + diff[1][0]
            xz = diff[0][2] + diff[2][0]
            yz = diff[1][2] + diff[2][1]
            size = jnp.sqrt(0.5 * own + 0.25 * (xy * xy + xz * xz + yz * yz) + strain_floor)
            omega = 1.0 / (base_tau + 3.0 * smag_coef * size)
            solid = solid_s[x, pl.ds(r, ROW), :] != 0
            density = rho_s[x, pl.ds(r, ROW), :]
            still = 1.0 - 1.5 * (u[0] * u[0] + u[1] * u[1] + u[2] * u[2])
            reads = [rd[k, x, pl.ds(r, ROW), :] for k in range(19)]
            scaled = {w: (w * density) * omega for w in sorted(set(WEIGHT))}
            keep = 1.0 - omega
            store(0, x, r, jnp.where(solid, reads[0], keep * reads[0] + scaled[WEIGHT[0]] * still))
            for k in range(1, 19, 2):
                other = OPP[k]
                project = None
                for c in range(3):
                    if CS[k][c]:
                        if project is None:
                            project = u[c] if CS[k][c] > 0 else -u[c]
                        else:
                            project = project + u[c] if CS[k][c] > 0 else project - u[c]
                even = still + 4.5 * project * project
                odd = 3.0 * project
                weight = scaled[WEIGHT[k]]
                store(k, x, r, jnp.where(solid, reads[other], keep * reads[k] + weight * (even + odd)))
                store(other, x, r, jnp.where(solid, reads[k], keep * reads[other] + weight * (even - odd)))

    def scale_of(tile):
        peak = jnp.max(jnp.max(tile, axis=0, keepdims=True), axis=1, keepdims=True)
        peak = jnp.broadcast_to(peak, (ROW, nz))
        return speed_cap / jnp.sqrt(speed_cap * speed_cap + peak)

    gone = []

    partners = (ngx - 1) + (ngy - 1) + 2 * (jnp.where(has_up, 1, 0) + jnp.where(has_down, 1, 0))
    load_p.wait()
    pl.semaphore_wait(barrier, partners)
    wait_a, sent = exchange(st0, a_send.at[0], a_recv.at[0], 8, moving)
    gone.append(sent)
    load_h.wait()
    load_o.wait()
    for x, r in blocks:
        rows = pl.ds(r, ROW)
        code = hl[x, rows, :]
        heat = jnp.zeros((ROW, nz), jnp.float32)
        for level in range(levels):
            heat = jnp.where(code == level, table[level], heat)
        grid_y = gy * sy + r + lax.broadcasted_iota(jnp.int32, (ROW, nz), 0)
        solid = (
            (ob[x, rows, :] == 1) | (grid_y == 0) | (grid_y == ngy * sy - 1) | first_lane | last_lane
        )
        solid_s[x, rows, :] = jnp.where(solid, 1, 0)
        v0[3, x + 1, pl.ds(ROW + r, ROW), :] = jnp.where(solid, 0.0, heat)
    wait_a()
    peak = streamed(st0, None)

    wait_b, sent = exchange(v0, b_send.at[0], b_recv.at[0], 4, lambda direction: [pl.ds(0, 4)])
    gone.append(sent)
    wait_y, sent = spread(0, 0, peak, pm_gy)
    gone.append(sent)
    wait_b()
    wait_x, sent = spread(0, 1, wait_y(), pm_gx)
    gone.append(sent)

    def store_st1(k, x, r, value):
        st1[k, x + 1, pl.ds(ROW + r, ROW), :] = value

    collided(v0, store_st1)

    wait_a, sent = exchange(st1, a_send.at[1], a_recv.at[1], 8, moving)
    gone.append(sent)
    fs = scale_of(wait_x())
    wait_a()
    peak = streamed(st1, fs)

    wait_b, sent = exchange(v1, b_send.at[1], b_recv.at[1], 4, lambda direction: [pl.ds(0, 3)])
    gone.append(sent)
    wait_y, sent = spread(1, 0, peak, pm_gy)
    gone.append(sent)
    send_v = pltpu.make_async_copy(v1.at[:, own_x, own_y, :], out_v, out_sem.at[19])
    send_v.start()
    wait_b()
    wait_x, sent = spread(1, 1, wait_y(), pm_gx)
    gone.append(sent)

    def store_out(k, x, r, value):
        obuf[k, x, pl.ds(r, ROW), :] = value

    collided(v1, store_out)
    outs = {k: pltpu.make_async_copy(obuf.at[k], out_p.at[k], out_sem.at[k]) for k in range(19)}
    for k in FLAT:
        outs[k].start()
    fs = scale_of(wait_x())
    lift = {(x, r): fs * v0[3, x + 1, pl.ds(ROW + r, ROW), :] for x, r in blocks}
    for k in LIFTED:
        for x, r in blocks:
            rows = pl.ds(r, ROW)
            obuf[k, x, rows, :] = obuf[k, x, rows, :] + (3.0 * WEIGHT[k] * CS[k][2]) * lift[(x, r)]
        outs[k].start()
    for sent in gone:
        sent()
    send_v.wait()
    for k in range(19):
        outs[k].wait()


def local(populations, heat_level, obstacle, heat_table):
    ngx = lax.axis_size("gx")
    ngy = lax.axis_size("gy")
    _, sx, sy, nz = populations.shape
    f32 = jnp.float32
    wide = (sx + 2, sy + 2 * ROW, nz)
    dma = pltpu.SemaphoreType.DMA
    return pl.pallas_call(
        functools.partial(kernel, ngx, ngy),
        out_shape=(
            jax.ShapeDtypeStruct(populations.shape, f32),
            jax.ShapeDtypeStruct((3, sx, sy, nz), f32),
        ),
        in_specs=[pl.BlockSpec(memory_space=pl.ANY)] * 3 + [pl.BlockSpec(memory_space=pltpu.SMEM)],
        out_specs=[pl.BlockSpec(memory_space=pl.ANY)] * 2,
        scratch_shapes=[
            pltpu.VMEM((19,) + wide, f32),
            pltpu.VMEM((19,) + wide, f32),
            pltpu.VMEM((19, sx, sy, nz), f32),
            pltpu.VMEM((sx, sy, nz), f32),
            pltpu.VMEM((4,) + wide, f32),
            pltpu.VMEM((3,) + wide, f32),
            pltpu.VMEM((sx, sy, nz), jnp.int32),
            pltpu.VMEM((sx, sy, nz), jnp.int32),
            pltpu.VMEM((sx, sy, nz), jnp.int32),
            pltpu.VMEM((19, sx, sy, nz), f32),
            pltpu.VMEM((STEPS, 2, ROW, nz), f32),
            pltpu.VMEM((STEPS, ngy - 1, ROW, nz), f32),
            pltpu.VMEM((STEPS, ngx - 1, ROW, nz), f32),
            dma((3,)),
            dma((STEPS, 8)),
            dma((STEPS, 8)),
            dma((STEPS, 4)),
            dma((STEPS, 4)),
            dma((STEPS, 2)),
            dma((STEPS, 2)),
            dma((20,)),
        ],
        compiler_params=pltpu.CompilerParams(collective_id=0, has_side_effects=True),
        name="lattice_steps",
    )(populations, heat_level, obstacle, heat_table)


def solution(mesh):
    return jax.shard_map(
        local,
        mesh=mesh,
        in_specs=(
            P(None, ("member", "gx"), "gy", None),
            P(("member", "gx"), "gy", None),
            P(("member", "gx"), "gy", None),
            P(),
        ),
        out_specs=(P(None, ("member", "gx"), "gy", None), P(None, ("member", "gx"), "gy", None)),
        check_vma=False,
    )
```

```python
import functools

import jax
import jax.numpy as jnp
import numpy as np
from jax import lax
from jax.experimental import pallas as pl
from jax.experimental.pallas import tpu as pltpu
from jax.sharding import PartitionSpec as P

STEPS = 2
ROW = 8

lattice = np.array(
    [
        [0, 0, 0],
        [1, 0, 0],
        [-1, 0, 0],
        [0, 1, 0],
        [0, -1, 0],
        [0, 0, 1],
        [0, 0, -1],
        [1, 1, 0],
        [-1, -1, 0],
        [1, -1, 0],
        [-1, 1, 0],
        [1, 0, 1],
        [-1, 0, -1],
        [1, 0, -1],
        [-1, 0, 1],
        [0, 1, 1],
        [0, -1, -1],
        [0, 1, -1],
        [0, -1, 1],
    ]
)
CS = [tuple(int(c) for c in row) for row in lattice]
WEIGHT = [1.0 / 3.0] + [1.0 / 18.0] * 6 + [1.0 / 36.0] * 12
OPP = [0, 2, 1, 4, 3, 6, 5, 8, 7, 10, 9, 12, 11, 14, 13, 16, 15, 18, 17]
base_tau = 0.52
smag_coef = 0.04
speed_cap = 0.1
strain_floor = 1e-06
LIFTED = [k for k in range(19) if CS[k][2] != 0]


def tree_sum(items):
    items = list(items)
    while len(items) > 1:
        items = [items[i] + items[i + 1] if i + 1 < len(items) else items[i] for i in range(0, len(items), 2)]
    return items[0]


def peak_groups(ngx, ngy):
    if ngx * ngy <= 64:
        return [[(dx, dy) for dx in range(ngx) for dy in range(ngy) if dx or dy]]
    return [[(0, dy) for dy in range(1, ngy)], [(dx, 0) for dx in range(1, ngx)]]


def kernel(
    ngx, ngy,
    pops, heat_level, obstacle, table,
    out_p, out_v,
    st0, st1, rd, rho_s, v0, v1, hl, ob, tb, solid_s, pm_src, *rest,
):
    *pm_bufs, load_sem, a_send, a_recv, b_send, b_recv, p_send, p_recv = rest
    _, sx, sy, nz = pops.shape
    levels = table.shape[0]
    gx = lax.axis_index("gx")
    gy = lax.axis_index("gy")
    has_up = gy < ngy - 1
    has_down = gy > 0
    right = lax.rem(gx + 1, ngx)
    left = lax.rem(gx + ngx - 1, ngx)
    own_x = pl.ds(1, sx)
    own_y = pl.ds(ROW, sy)
    top = pl.ds(ROW + sy - 1, 1)
    bottom = pl.ds(ROW, 1)
    rim_low = pl.ds(ROW - 1, 1)
    rim_high = pl.ds(ROW + sy, 1)

    load_p = pltpu.make_async_copy(pops, st0.at[:, own_x, own_y, :], load_sem.at[0])
    load_h = pltpu.make_async_copy(heat_level, hl, load_sem.at[1])
    load_o = pltpu.make_async_copy(obstacle, ob, load_sem.at[2])
    load_p.start()
    load_h.start()
    load_o.start()
    load_t = pltpu.make_async_copy(table, tb, load_sem.at[3])
    load_t.start()

    barrier = pltpu.get_barrier_semaphore()

    def greet(x, y):
        pl.semaphore_signal(barrier, inc=1, device_id={"gx": x, "gy": y}, device_id_type=pl.DeviceIdType.MESH)

    groups = peak_groups(ngx, ngy)
    partners = sum(len(group) for group in groups)
    for group in groups:
        for dx, dy in group:
            greet(lax.rem(gx + dx, ngx), lax.rem(gy + dy, ngy))
    if len(groups) > 1:
        partners = partners + 2 * (jnp.where(has_up, 1, 0) + jnp.where(has_down, 1, 0))

        @pl.when(has_up)
        def _():
            greet(right, gy + 1)
            greet(left, gy + 1)

        @pl.when(has_down)
        def _():
            greet(right, gy - 1)
            greet(left, gy - 1)

    def zero_rim(rows):
        for ref in (st0, st1, v0, v1):
            ref[:, :, rows, :] = jnp.zeros((ref.shape[0], sx + 2, 1, nz), jnp.float32)

    @pl.when(jnp.logical_not(has_down))
    def _():
        zero_rim(rim_low)

    @pl.when(jnp.logical_not(has_up))
    def _():
        zero_rim(rim_high)

    sides = (
        (None, right, gy, (1, 0)),
        (None, left, gy, (-1, 0)),
        (has_up, gx, gy + 1, (0, 1)),
        (has_down, gx, gy - 1, (0, -1)),
        (has_up, right, gy + 1, (1, 1)),
        (has_down, left, gy - 1, (-1, -1)),
        (has_down, right, gy - 1, (1, -1)),
        (has_up, left, gy + 1, (-1, 1)),
    )
    arrives = (None, None, has_down, has_up, has_down, has_up, has_up, has_down)

    def src_dst(direction):
        dx, dy = direction
        xs = {1: (sx, 0), -1: (1, sx + 1), 0: (own_x, own_x)}[dx]
        ys = {1: (top, rim_low), -1: (bottom, rim_high), 0: (own_y, own_y)}[dy]
        return (xs[0], ys[0]), (xs[1], ys[1])

    def guarded(cond, fn):
        if cond is None:
            fn()
        else:
            pl.when(cond)(fn)

    def moving(direction):
        dx, dy = direction
        if dx and dy:
            return [k for k in range(19) if CS[k][:2] == direction]
        return [k for k in range(19) if (CS[k][0] == dx if dx else CS[k][1] == dy)]

    def exchange(ref, send, recv, many, groups):
        def start(number, x, y, direction):
            def go():
                s, d = src_dst(direction)
                for g in groups(direction):
                    pltpu.make_async_remote_copy(
                        src_ref=ref.at[g, s[0], s[1], :],
                        dst_ref=ref.at[g, d[0], d[1], :],
                        send_sem=send.at[number],
                        recv_sem=recv.at[number],
                        device_id={"gx": x, "gy": y},
                        device_id_type=pl.DeviceIdType.MESH,
                    ).start()
            return go

        for number, (cond, x, y, direction) in enumerate(sides[:many]):
            guarded(cond, start(number, x, y, direction))

        def total(number, direction, sem):
            def go():
                s, _ = src_dst(direction)
                gs = groups(direction)
                view = ref.at[pl.ds(0, len(gs)) if isinstance(gs[0], int) else gs[0], s[0], s[1], :]
                pltpu.make_async_copy(view, view, sem.at[number]).wait()
            return go

        def wait_recv():
            for number in range(many):
                guarded(arrives[number], total(number, sides[number][3], recv))

        def wait_send():
            for number in range(many):
                guarded(sides[number][0], total(number, sides[number][3], send))

        return wait_recv, wait_send

    def spread(step, phase, value):
        group = peak_groups(ngx, ngy)[phase]
        count = len(group)
        buf = pm_bufs[phase]
        pm_src[step, phase] = value
        for d, (dx, dy) in enumerate(group, 1):
            place = {"gx": lax.rem(gx + dx, ngx), "gy": lax.rem(gy + dy, ngy)}
            pltpu.make_async_remote_copy(
                src_ref=pm_src.at[step, phase],
                dst_ref=buf.at[step, d - 1],
                send_sem=p_send.at[step, phase],
                recv_sem=p_recv.at[step, phase],
                device_id=place,
                device_id_type=pl.DeviceIdType.MESH,
            ).start()

        def wait():
            pltpu.make_async_copy(buf.at[step], buf.at[step], p_recv.at[step, phase]).wait()
            best = value
            for d in range(count):
                best = jnp.maximum(best, buf[step, d])
            return best

        def wait_send():
            pltpu.make_async_copy(buf.at[step], buf.at[step], p_send.at[step, phase]).wait()

        return wait, wait_send

    blocks = [(x, r) for x in range(sx) for r in range(0, sy, ROW)]
    lane = lax.broadcasted_iota(jnp.int32, (ROW, nz), 1)
    first_lane = lane == 0
    last_lane = lane == nz - 1

    def streamed(st, fs):
        peak = jnp.zeros((ROW, nz), jnp.float32)
        vel = v0 if st is st0 else v1
        for x, r in blocks:
            reads = []
            for k, (cx, cy, cz) in enumerate(CS):
                rows = pl.ds(ROW + r - cy, ROW)
                cells = st[k, x + 1 - cx, rows, :]
                if cz:
                    if fs is not None:
                        cells = cells + (3.0 * WEIGHT[k] * cz) * (fs * v0[3, x + 1 - cx, rows, :])
                    cells = pltpu.roll(cells, cz % nz, 1)
                    cells = jnp.where(first_lane if cz > 0 else last_lane, 0.0, cells)
                rd[k, x, pl.ds(r, ROW), :] = cells
                reads.append(cells)
            density = tree_sum(reads)
            solid = solid_s[x, pl.ds(r, ROW), :] != 0
            inv = jnp.where(solid, 0.0, 1.0 / jnp.where(solid, 1.0, density))
            rho_s[x, pl.ds(r, ROW), :] = density
            speed = []
            for c in range(3):
                plus = tree_sum([reads[k] for k in range(19) if CS[k][c] > 0])
                minus = tree_sum([reads[k] for k in range(19) if CS[k][c] < 0])
                u = (plus - minus) * inv
                vel[c, x + 1, pl.ds(ROW + r, ROW), :] = u
                speed.append(u * u)
            peak = jnp.maximum(peak, speed[0] + speed[1] + speed[2])
        return peak

    def collided(vel, store):
        for x, r in blocks:
            mid = pl.ds(ROW + r, ROW)
            u = [vel[c, x + 1, mid, :] for c in range(3)]
            diff = []
            for a in range(3):
                diff.append(
                    (
                        vel[a, x + 2, mid, :] - vel[a, x, mid, :],
                        vel[a, x + 1, pl.ds(ROW + r + 1, ROW), :] - vel[a, x + 1, pl.ds(ROW + r - 1, ROW), :],
                        pltpu.roll(u[a], nz - 1, 1) - pltpu.roll(u[a], 1, 1),
                    )
                )
            own = diff[0][0] * diff[0][0] + diff[1][1] * diff[1][1] + diff[2][2] * diff[2][2]
            xy = diff[0][1] + diff[1][0]
            xz = diff[0][2] + diff[2][0]
            yz = diff[1][2] + diff[2][1]
            size = jnp.sqrt(0.5 * own + 0.25 * (xy * xy + xz * xz + yz * yz) + strain_floor)
            omega = 1.0 / (base_tau + 3.0 * smag_coef * size)
            solid = solid_s[x, pl.ds(r, ROW), :] != 0
            density = rho_s[x, pl.ds(r, ROW), :]
            still = 1.0 - 1.5 * (u[0] * u[0] + u[1] * u[1] + u[2] * u[2])
            reads = [rd[k, x, pl.ds(r, ROW), :] for k in range(19)]
            scaled = {w: (w * density) * omega for w in sorted(set(WEIGHT))}
            keep = 1.0 - omega
            store(0, x, r, jnp.where(solid, reads[0], keep * reads[0] + scaled[WEIGHT[0]] * still))
            for k in range(1, 19, 2):
                other = OPP[k]
                project = None
                for c in range(3):
                    if CS[k][c]:
                        if project is None:
                            project = u[c] if CS[k][c] > 0 else -u[c]
                        else:
                            project = project + u[c] if CS[k][c] > 0 else project - u[c]
                even = still + 4.5 * project * project
                odd = 3.0 * project
                weight = scaled[WEIGHT[k]]
                store(k, x, r, jnp.where(solid, reads[other], keep * reads[k] + weight * (even + odd)))
                store(other, x, r, jnp.where(solid, reads[k], keep * reads[other] + weight * (even - odd)))

    def scale_of(tile):
        peak = jnp.max(jnp.max(tile, axis=0, keepdims=True), axis=1, keepdims=True)
        peak = jnp.broadcast_to(peak, (ROW, nz))
        return speed_cap / jnp.sqrt(speed_cap * speed_cap + peak)

    gone = []

    load_p.wait()
    pl.semaphore_wait(barrier, partners)
    wait_a, sent = exchange(st0, a_send.at[0], a_recv.at[0], 8, moving)
    gone.append(sent)
    load_h.wait()
    load_o.wait()
    load_t.wait()
    for x, r in blocks:
        rows = pl.ds(r, ROW)
        code = hl[x, rows, :]
        heat = jnp.zeros((ROW, nz), jnp.float32)
        for level in range(levels):
            heat = jnp.where(code == level, tb[level], heat)
        grid_y = gy * sy + r + lax.broadcasted_iota(jnp.int32, (ROW, nz), 0)
        solid = (
            (ob[x, rows, :] == 1) | (grid_y == 0) | (grid_y == ngy * sy - 1) | first_lane | last_lane
        )
        solid_s[x, rows, :] = jnp.where(solid, 1, 0)
        v0[3, x + 1, pl.ds(ROW + r, ROW), :] = jnp.where(solid, 0.0, heat)
    wait_a()
    peak = streamed(st0, None)

    wait_b, sent = exchange(v0, b_send.at[0], b_recv.at[0], 4, lambda direction: [pl.ds(0, 4)])
    gone.append(sent)
    wait_peak, sent = spread(0, 0, peak)
    gone.append(sent)
    wait_b()
    for phase in range(1, len(pm_bufs)):
        wait_peak, sent = spread(0, phase, wait_peak())
        gone.append(sent)

    def store_st1(k, x, r, value):
        st1[k, x + 1, pl.ds(ROW + r, ROW), :] = value

    collided(v0, store_st1)

    wait_a, sent = exchange(st1, a_send.at[1], a_recv.at[1], 8, moving)
    gone.append(sent)
    fs = scale_of(wait_peak())
    wait_a()
    peak = streamed(st1, fs)

    wait_b, sent = exchange(v1, b_send.at[1], b_recv.at[1], 4, lambda direction: [pl.ds(0, 3)])
    gone.append(sent)
    wait_peak, sent = spread(1, 0, peak)
    gone.append(sent)
    for x, r in blocks:
        for c in range(3):
            out_v[c, x, pl.ds(r, ROW), :] = v1[c, x + 1, pl.ds(ROW + r, ROW), :]
    wait_b()
    for phase in range(1, len(pm_bufs)):
        wait_peak, sent = spread(1, phase, wait_peak())
        gone.append(sent)

    def store_out(k, x, r, value):
        out_p[k, x, pl.ds(r, ROW), :] = value

    collided(v1, store_out)
    fs = scale_of(wait_peak())
    lift = {(x, r): fs * v0[3, x + 1, pl.ds(ROW + r, ROW), :] for x, r in blocks}
    for k in LIFTED:
        for x, r in blocks:
            rows = pl.ds(r, ROW)
            out_p[k, x, rows, :] = out_p[k, x, rows, :] + (3.0 * WEIGHT[k] * CS[k][2]) * lift[(x, r)]
    for sent in gone:
        sent()


def write_out(pops, vel, out_p, out_v, sems):
    copies = [
        pltpu.make_async_copy(pops, out_p, sems.at[0]),
        pltpu.make_async_copy(vel, out_v, sems.at[1]),
    ]
    for copy in copies:
        copy.start()
    for copy in copies:
        copy.wait()


def local(populations, heat_level, obstacle, heat_table):
    ngx = lax.axis_size("gx")
    ngy = lax.axis_size("gy")
    _, sx, sy, nz = populations.shape
    f32 = jnp.float32
    wide = (sx + 2, sy + 2 * ROW, nz)
    dma = pltpu.SemaphoreType.DMA
    groups = peak_groups(ngx, ngy)
    phases = len(groups)
    vmem = pl.BlockSpec(memory_space=pltpu.VMEM)
    anywhere = pl.BlockSpec(memory_space=pltpu.HBM)
    shapes = (
        jax.ShapeDtypeStruct(populations.shape, f32),
        jax.ShapeDtypeStruct((3, sx, sy, nz), f32),
    )
    pops, velocity = pl.pallas_call(
        functools.partial(kernel, ngx, ngy),
        out_shape=shapes,
        in_specs=[anywhere] * 4,
        out_specs=[vmem] * 2,
        scratch_shapes=[
            pltpu.VMEM((19,) + wide, f32),
            pltpu.VMEM((19,) + wide, f32),
            pltpu.VMEM((19, sx, sy, nz), f32),
            pltpu.VMEM((sx, sy, nz), f32),
            pltpu.VMEM((4,) + wide, f32),
            pltpu.VMEM((3,) + wide, f32),
            pltpu.VMEM((sx, sy, nz), jnp.int32),
            pltpu.VMEM((sx, sy, nz), jnp.int32),
            pltpu.SMEM(heat_table.shape, f32),
            pltpu.VMEM((sx, sy, nz), jnp.int32),
            pltpu.VMEM((STEPS, phases, ROW, nz), f32),
            *[pltpu.VMEM((STEPS, len(group), ROW, nz), f32) for group in groups],
            dma((4,)),
            dma((STEPS, 8)),
            dma((STEPS, 8)),
            dma((STEPS, 4)),
            dma((STEPS, 4)),
            dma((STEPS, phases)),
            dma((STEPS, phases)),
        ],
        compiler_params=pltpu.CompilerParams(
            collective_id=0, has_side_effects=True, vmem_limit_bytes=24 * 1024 * 1024
        ),
        name="lattice_steps",
    )(populations, heat_level, obstacle, heat_table)
    return pl.pallas_call(
        write_out,
        out_shape=shapes,
        in_specs=[vmem] * 2,
        out_specs=[anywhere] * 2,
        scratch_shapes=[dma((2,))],
        compiler_params=pltpu.CompilerParams(vmem_limit_bytes=8 * 1024 * 1024),
        name="write_out",
    )(pops, velocity)


def solution(mesh):
    return jax.shard_map(
        local,
        mesh=mesh,
        in_specs=(
            P(None, ("member", "gx"), "gy", None),
            P(("member", "gx"), "gy", None),
            P(("member", "gx"), "gy", None),
            P(),
        ),
        out_specs=(P(None, ("member", "gx"), "gy", None), P(None, ("member", "gx"), "gy", None)),
        check_vma=False,
    )
```

```python
import functools

import jax
import jax.numpy as jnp
import numpy as np
from jax import lax
from jax.experimental import pallas as pl
from jax.experimental.pallas import tpu as pltpu
from jax.sharding import PartitionSpec as P

STEPS = 2
ROW = 8

lattice = np.array(
    [
        [0, 0, 0],
        [1, 0, 0],
        [-1, 0, 0],
        [0, 1, 0],
        [0, -1, 0],
        [0, 0, 1],
        [0, 0, -1],
        [1, 1, 0],
        [-1, -1, 0],
        [1, -1, 0],
        [-1, 1, 0],
        [1, 0, 1],
        [-1, 0, -1],
        [1, 0, -1],
        [-1, 0, 1],
        [0, 1, 1],
        [0, -1, -1],
        [0, 1, -1],
        [0, -1, 1],
    ]
)
CS = [tuple(int(c) for c in row) for row in lattice]
WEIGHT = [1.0 / 3.0] + [1.0 / 18.0] * 6 + [1.0 / 36.0] * 12
OPP = [0, 2, 1, 4, 3, 6, 5, 8, 7, 10, 9, 12, 11, 14, 13, 16, 15, 18, 17]
base_tau = 0.52
smag_coef = 0.04
speed_cap = 0.1
strain_floor = 1e-06
LIFTED = [k for k in range(19) if CS[k][2] != 0]


def tree_sum(items):
    items = list(items)
    while len(items) > 1:
        items = [items[i] + items[i + 1] if i + 1 < len(items) else items[i] for i in range(0, len(items), 2)]
    return items[0]


def peak_groups(ngx, ngy):
    if ngx * ngy <= 64:
        return [[(dx, dy) for dx in range(ngx) for dy in range(ngy) if dx or dy]]
    return [[(0, dy) for dy in range(1, ngy)], [(dx, 0) for dx in range(1, ngx)]]


def kernel(
    ngx, ngy,
    pops, heat_level, obstacle, table,
    out_p, out_v,
    st0, st1, rd, rho_s, v0, v1, hl, ob, tb, solid_s, pm_src, *rest,
):
    *pm_bufs, load_sem, a_send, a_recv, b_send, b_recv, p_send, p_recv = rest
    _, sx, sy, nz = pops.shape
    levels = table.shape[0]
    gx = lax.axis_index("gx")
    gy = lax.axis_index("gy")
    has_up = gy < ngy - 1
    has_down = gy > 0
    right = lax.rem(gx + 1, ngx)
    left = lax.rem(gx + ngx - 1, ngx)
    own_x = pl.ds(1, sx)
    own_y = pl.ds(ROW, sy)
    top = pl.ds(ROW + sy - 1, 1)
    bottom = pl.ds(ROW, 1)
    rim_low = pl.ds(ROW - 1, 1)
    rim_high = pl.ds(ROW + sy, 1)

    load_p = pltpu.make_async_copy(pops, st0.at[:, own_x, own_y, :], load_sem.at[0])
    load_h = pltpu.make_async_copy(heat_level, hl, load_sem.at[1])
    load_o = pltpu.make_async_copy(obstacle, ob, load_sem.at[2])
    load_p.start()
    load_h.start()
    load_o.start()
    load_t = pltpu.make_async_copy(table, tb, load_sem.at[3])
    load_t.start()

    barrier = pltpu.get_barrier_semaphore()

    def greet(x, y):
        pl.semaphore_signal(barrier, inc=1, device_id={"gx": x, "gy": y}, device_id_type=pl.DeviceIdType.MESH)

    groups = peak_groups(ngx, ngy)
    partners = sum(len(group) for group in groups)
    for group in groups:
        for dx, dy in group:
            greet(lax.rem(gx + dx, ngx), lax.rem(gy + dy, ngy))
    if len(groups) > 1:
        partners = partners + 2 * (jnp.where(has_up, 1, 0) + jnp.where(has_down, 1, 0))

        @pl.when(has_up)
        def _():
            greet(right, gy + 1)
            greet(left, gy + 1)

        @pl.when(has_down)
        def _():
            greet(right, gy - 1)
            greet(left, gy - 1)

    def zero_rim(rows):
        for ref in (st0, st1, v0, v1):
            ref[:, :, rows, :] = jnp.zeros((ref.shape[0], sx + 2, 1, nz), jnp.float32)

    @pl.when(jnp.logical_not(has_down))
    def _():
        zero_rim(rim_low)

    @pl.when(jnp.logical_not(has_up))
    def _():
        zero_rim(rim_high)

    sides = (
        (None, right, gy, (1, 0)),
        (None, left, gy, (-1, 0)),
        (has_up, gx, gy + 1, (0, 1)),
        (has_down, gx, gy - 1, (0, -1)),
        (has_up, right, gy + 1, (1, 1)),
        (has_down, left, gy - 1, (-1, -1)),
        (has_down, right, gy - 1, (1, -1)),
        (has_up, left, gy + 1, (-1, 1)),
    )
    arrives = (None, None, has_down, has_up, has_down, has_up, has_up, has_down)

    def src_dst(direction):
        dx, dy = direction
        xs = {1: (sx, 0), -1: (1, sx + 1), 0: (own_x, own_x)}[dx]
        ys = {1: (top, rim_low), -1: (bottom, rim_high), 0: (own_y, own_y)}[dy]
        return (xs[0], ys[0]), (xs[1], ys[1])

    def guarded(cond, fn):
        if cond is None:
            fn()
        else:
            pl.when(cond)(fn)

    def moving(direction):
        dx, dy = direction
        if dx and dy:
            return [k for k in range(19) if CS[k][:2] == direction]
        return [k for k in range(19) if (CS[k][0] == dx if dx else CS[k][1] == dy)]

    def exchange(ref, send, recv, many, groups):
        def start(number, x, y, direction):
            def go():
                s, d = src_dst(direction)
                for g in groups(direction):
                    pltpu.make_async_remote_copy(
                        src_ref=ref.at[g, s[0], s[1], :],
                        dst_ref=ref.at[g, d[0], d[1], :],
                        send_sem=send.at[number],
                        recv_sem=recv.at[number],
                        device_id={"gx": x, "gy": y},
                        device_id_type=pl.DeviceIdType.MESH,
                    ).start()
            return go

        for number, (cond, x, y, direction) in enumerate(sides[:many]):
            guarded(cond, start(number, x, y, direction))

        def total(number, direction, sem):
            def go():
                s, _ = src_dst(direction)
                gs = groups(direction)
                view = ref.at[pl.ds(0, len(gs)) if isinstance(gs[0], int) else gs[0], s[0], s[1], :]
                pltpu.make_async_copy(view, view, sem.at[number]).wait()
            return go

        def wait_recv():
            for number in range(many):
                guarded(arrives[number], total(number, sides[number][3], recv))

        def wait_send():
            for number in range(many):
                guarded(sides[number][0], total(number, sides[number][3], send))

        return wait_recv, wait_send

    def spread(step, phase, value):
        group = peak_groups(ngx, ngy)[phase]
        count = len(group)
        buf = pm_bufs[phase]
        pm_src[step, phase] = value
        for d, (dx, dy) in enumerate(group, 1):
            place = {"gx": lax.rem(gx + dx, ngx), "gy": lax.rem(gy + dy, ngy)}
            pltpu.make_async_remote_copy(
                src_ref=pm_src.at[step, phase],
                dst_ref=buf.at[step, d - 1],
                send_sem=p_send.at[step, phase],
                recv_sem=p_recv.at[step, phase],
                device_id=place,
                device_id_type=pl.DeviceIdType.MESH,
            ).start()

        def wait():
            pltpu.make_async_copy(buf.at[step], buf.at[step], p_recv.at[step, phase]).wait()
            best = value
            for d in range(count):
                best = jnp.maximum(best, buf[step, d])
            return best

        def wait_send():
            pltpu.make_async_copy(buf.at[step], buf.at[step], p_send.at[step, phase]).wait()

        return wait, wait_send

    blocks = [(x, r) for x in range(sx) for r in range(0, sy, ROW)]
    lane = lax.broadcasted_iota(jnp.int32, (ROW, nz), 1)
    first_lane = lane == 0
    last_lane = lane == nz - 1

    def streamed(st, fs):
        peak = jnp.zeros((ROW, nz), jnp.float32)
        vel = v0 if st is st0 else v1
        for x, r in blocks:
            reads = []
            for k, (cx, cy, cz) in enumerate(CS):
                rows = pl.ds(ROW + r - cy, ROW)
                cells = st[k, x + 1 - cx, rows, :]
                if cz:
                    if fs is not None:
                        cells = cells + (3.0 * WEIGHT[k] * cz) * (fs * v0[3, x + 1 - cx, rows, :])
                    cells = pltpu.roll(cells, cz % nz, 1)
                    cells = jnp.where(first_lane if cz > 0 else last_lane, 0.0, cells)
                rd[k, x, pl.ds(r, ROW), :] = cells
                reads.append(cells)
            density = tree_sum(reads)
            solid = solid_s[x, pl.ds(r, ROW), :] != 0
            inv = jnp.where(solid, 0.0, 1.0 / jnp.where(solid, 1.0, density))
            rho_s[x, pl.ds(r, ROW), :] = density
            speed = []
            for c in range(3):
                plus = tree_sum([reads[k] for k in range(19) if CS[k][c] > 0])
                minus = tree_sum([reads[k] for k in range(19) if CS[k][c] < 0])
                u = (plus - minus) * inv
                vel[c, x + 1, pl.ds(ROW + r, ROW), :] = u
                speed.append(u * u)
            peak = jnp.maximum(peak, speed[0] + speed[1] + speed[2])
        return peak

    def collided(vel, store):
        for x, r in blocks:
            mid = pl.ds(ROW + r, ROW)
            u = [vel[c, x + 1, mid, :] for c in range(3)]
            diff = []
            for a in range(3):
                diff.append(
                    (
                        vel[a, x + 2, mid, :] - vel[a, x, mid, :],
                        vel[a, x + 1, pl.ds(ROW + r + 1, ROW), :] - vel[a, x + 1, pl.ds(ROW + r - 1, ROW), :],
                        pltpu.roll(u[a], nz - 1, 1) - pltpu.roll(u[a], 1, 1),
                    )
                )
            own = diff[0][0] * diff[0][0] + diff[1][1] * diff[1][1] + diff[2][2] * diff[2][2]
            xy = diff[0][1] + diff[1][0]
            xz = diff[0][2] + diff[2][0]
            yz = diff[1][2] + diff[2][1]
            size = jnp.sqrt(0.5 * own + 0.25 * (xy * xy + xz * xz + yz * yz) + strain_floor)
            omega = 1.0 / (base_tau + 3.0 * smag_coef * size)
            solid = solid_s[x, pl.ds(r, ROW), :] != 0
            density = rho_s[x, pl.ds(r, ROW), :]
            still = 1.0 - 1.5 * (u[0] * u[0] + u[1] * u[1] + u[2] * u[2])
            reads = [rd[k, x, pl.ds(r, ROW), :] for k in range(19)]
            scaled = {w: (w * density) * omega for w in sorted(set(WEIGHT))}
            keep = 1.0 - omega
            store(0, x, r, jnp.where(solid, reads[0], keep * reads[0] + scaled[WEIGHT[0]] * still))
            for k in range(1, 19, 2):
                other = OPP[k]
                project = None
                for c in range(3):
                    if CS[k][c]:
                        if project is None:
                            project = u[c] if CS[k][c] > 0 else -u[c]
                        else:
                            project = project + u[c] if CS[k][c] > 0 else project - u[c]
                even = still + 4.5 * project * project
                odd = 3.0 * project
                weight = scaled[WEIGHT[k]]
                store(k, x, r, jnp.where(solid, reads[other], keep * reads[k] + weight * (even + odd)))
                store(other, x, r, jnp.where(solid, reads[k], keep * reads[other] + weight * (even - odd)))

    def scale_of(tile):
        peak = jnp.max(jnp.max(tile, axis=0, keepdims=True), axis=1, keepdims=True)
        peak = jnp.broadcast_to(peak, (ROW, nz))
        return speed_cap / jnp.sqrt(speed_cap * speed_cap + peak)

    gone = []

    load_p.wait()
    pl.semaphore_wait(barrier, partners)
    wait_a, sent = exchange(st0, a_send.at[0], a_recv.at[0], 8, moving)
    gone.append(sent)
    load_h.wait()
    load_o.wait()
    load_t.wait()
    for x, r in blocks:
        rows = pl.ds(r, ROW)
        code = hl[x, rows, :]
        heat = jnp.zeros((ROW, nz), jnp.float32)
        for level in range(levels):
            heat = jnp.where(code == level, tb[level], heat)
        grid_y = gy * sy + r + lax.broadcasted_iota(jnp.int32, (ROW, nz), 0)
        solid = (
            (ob[x, rows, :] == 1) | (grid_y == 0) | (grid_y == ngy * sy - 1) | first_lane | last_lane
        )
        solid_s[x, rows, :] = jnp.where(solid, 1, 0)
        v0[3, x + 1, pl.ds(ROW + r, ROW), :] = jnp.where(solid, 0.0, heat)
    wait_a()
    peak = streamed(st0, None)

    wait_b, sent = exchange(v0, b_send.at[0], b_recv.at[0], 4, lambda direction: [pl.ds(0, 4)])
    gone.append(sent)
    wait_peak, sent = spread(0, 0, peak)
    gone.append(sent)
    wait_b()
    for phase in range(1, len(pm_bufs)):
        wait_peak, sent = spread(0, phase, wait_peak())
        gone.append(sent)

    def store_st1(k, x, r, value):
        st1[k, x + 1, pl.ds(ROW + r, ROW), :] = value

    collided(v0, store_st1)

    wait_a, sent = exchange(st1, a_send.at[1], a_recv.at[1], 8, moving)
    gone.append(sent)
    fs = scale_of(wait_peak())
    wait_a()
    peak = streamed(st1, fs)

    wait_b, sent = exchange(v1, b_send.at[1], b_recv.at[1], 4, lambda direction: [pl.ds(0, 3)])
    gone.append(sent)
    wait_peak, sent = spread(1, 0, peak)
    gone.append(sent)
    for x, r in blocks:
        for c in range(3):
            out_v[c, x, pl.ds(r, ROW), :] = v1[c, x + 1, pl.ds(ROW + r, ROW), :]
    wait_b()
    for phase in range(1, len(pm_bufs)):
        wait_peak, sent = spread(1, phase, wait_peak())
        gone.append(sent)

    def store_out(k, x, r, value):
        out_p[k, x, pl.ds(r, ROW), :] = value

    collided(v1, store_out)
    fs = scale_of(wait_peak())
    lift = {(x, r): fs * v0[3, x + 1, pl.ds(ROW + r, ROW), :] for x, r in blocks}
    for k in LIFTED:
        for x, r in blocks:
            rows = pl.ds(r, ROW)
            out_p[k, x, rows, :] = out_p[k, x, rows, :] + (3.0 * WEIGHT[k] * CS[k][2]) * lift[(x, r)]
    for sent in gone:
        sent()


def write_out(pops, vel, out_p, out_v, sems):
    copies = [
        pltpu.make_async_copy(pops, out_p, sems.at[0]),
        pltpu.make_async_copy(vel, out_v, sems.at[1]),
    ]
    for copy in copies:
        copy.start()
    for copy in copies:
        copy.wait()


def local(populations, heat_level, obstacle, heat_table):
    ngx = lax.axis_size("gx")
    ngy = lax.axis_size("gy")
    _, sx, sy, nz = populations.shape
    f32 = jnp.float32
    wide = (sx + 2, sy + 2 * ROW, nz)
    dma = pltpu.SemaphoreType.DMA
    groups = peak_groups(ngx, ngy)
    phases = len(groups)
    vmem = pl.BlockSpec(memory_space=pltpu.VMEM)
    anywhere = pl.BlockSpec(memory_space=pltpu.HBM)
    shapes = (
        jax.ShapeDtypeStruct(populations.shape, f32),
        jax.ShapeDtypeStruct((3, sx, sy, nz), f32),
    )
    pops, velocity = pl.pallas_call(
        functools.partial(kernel, ngx, ngy),
        out_shape=shapes,
        in_specs=[anywhere] * 4,
        out_specs=[vmem] * 2,
        scratch_shapes=[
            pltpu.VMEM((19,) + wide, f32),
            pltpu.VMEM((19,) + wide, f32),
            pltpu.VMEM((19, sx, sy, nz), f32),
            pltpu.VMEM((sx, sy, nz), f32),
            pltpu.VMEM((4,) + wide, f32),
            pltpu.VMEM((3,) + wide, f32),
            pltpu.VMEM((sx, sy, nz), jnp.int32),
            pltpu.VMEM((sx, sy, nz), jnp.int32),
            pltpu.SMEM(heat_table.shape, f32),
            pltpu.VMEM((sx, sy, nz), jnp.int32),
            pltpu.VMEM((STEPS, phases, ROW, nz), f32),
            *[pltpu.VMEM((STEPS, len(group), ROW, nz), f32) for group in groups],
            dma((4,)),
            dma((STEPS, 8)),
            dma((STEPS, 8)),
            dma((STEPS, 4)),
            dma((STEPS, 4)),
            dma((STEPS, phases)),
            dma((STEPS, phases)),
        ],
        compiler_params=pltpu.CompilerParams(
            collective_id=0, has_side_effects=True, vmem_limit_bytes=24 * 1024 * 1024
        ),
        name="lattice_steps",
    )(*[pltpu.with_memory_space_constraint(a, pltpu.HBM) for a in (populations, heat_level, obstacle, heat_table)])
    return pl.pallas_call(
        write_out,
        out_shape=shapes,
        in_specs=[vmem] * 2,
        out_specs=[anywhere] * 2,
        scratch_shapes=[dma((2,))],
        compiler_params=pltpu.CompilerParams(vmem_limit_bytes=8 * 1024 * 1024),
        name="write_out",
    )(pops, velocity)


def solution(mesh):
    return jax.shard_map(
        local,
        mesh=mesh,
        in_specs=(
            P(None, ("member", "gx"), "gy", None),
            P(("member", "gx"), "gy", None),
            P(("member", "gx"), "gy", None),
            P(),
        ),
        out_specs=(P(None, ("member", "gx"), "gy", None), P(None, ("member", "gx"), "gy", None)),
        check_vma=False,
    )
```
